8 devices in a mesh: dp: 1 (over z), tp: 2 (over y), ep: 4 (over x, core).
Axes of the slice: x: 2, y: 2, z: 1, core: 2. Of those that a mesh axis runs over, the one named last changes fastest.
Arguments:
- tokens: bfloat16 [256, 2048], P(('dp', 'ep'))
- expert_ids: int32 [256, 8], P(('dp', 'ep'))
- norm_gain: bfloat16 [2048], replicated
- router_w: bfloat16 [2048, 64], replicated
- w_gate: bfloat16 [64, 2048, 1024], P('ep', None, 'tp')
- w_up: bfloat16 [64, 2048, 1024], P('ep', None, 'tp')
- w_down: bfloat16 [64, 1024, 2048], P('ep', 'tp')
Outputs:
- output: bfloat16 [256, 2048], P(('dp', 'ep'))
All inputs are finite; a program needn't handle non-finite values.
Results may differ from the reference program's by a relative error of at most 0.0102047.
Values are sent between devices in bfloat16 or wider.
A program may use at most 1 GiB of HBM per device.

```python
import jax
import jax.numpy as jnp
from jax import lax

MODEL_DIM = 2048
FFN_DIM = 1024
NUM_EXPERTS = 64
TOP_K = 8
EP_SIZE = 4
TOK_DEV = 64
TOKENS = EP_SIZE * TOK_DEV
SLOT_CAP = 2 * TOP_K * TOK_DEV // NUM_EXPERTS
EXPERT_CAP = EP_SIZE * SLOT_CAP
NORM_EPS = 1e-5


def route_block(key):
    mean_load = TOP_K * TOK_DEV // NUM_EXPERTS
    key_lift, key_perm, key_tok = jax.random.split(key, 3)
    lifts = jax.random.randint(key_lift, (NUM_EXPERTS,), 1, mean_load, jnp.int32)
    lifts = lifts.at[0].set(mean_load).at[1].set(0)
    loads = mean_load + lifts - jnp.roll(lifts, -1)
    order = jnp.repeat(jnp.arange(NUM_EXPERTS, dtype=jnp.int32), loads, total_repeat_length=TOP_K * TOK_DEV)
    choice = order.reshape(TOP_K, TOK_DEV).T
    relabel = jax.random.permutation(key_perm, NUM_EXPERTS).astype(jnp.int32)
    shuffle = jax.random.permutation(key_tok, TOK_DEV)
    return relabel[choice][shuffle]


def setup_inputs(seed: int = 0, part: int = 0) -> dict:
    keys = jax.random.split(jax.random.key(seed), 5)
    tok_key = jax.random.fold_in(jax.random.key(seed + 1), part)
    route_key = jax.random.fold_in(jax.random.key(seed + 2), part)
    tokens = jax.random.normal(tok_key, (TOKENS, MODEL_DIM), jnp.float32)
    expert_ids = jax.vmap(route_block)(jax.random.split(route_key, EP_SIZE)).reshape(TOKENS, TOP_K)
    norm_gain = 1.0 + 0.5 * jax.random.normal(keys[0], (MODEL_DIM,), jnp.float32)
    router_w = jax.random.normal(keys[1], (MODEL_DIM, NUM_EXPERTS), jnp.float32) * MODEL_DIM ** -0.5
    w_gate = jax.random.normal(keys[2], (NUM_EXPERTS, MODEL_DIM, FFN_DIM), jnp.float32) * MODEL_DIM ** -0.5
    w_up = jax.random.normal(keys[3], (NUM_EXPERTS, MODEL_DIM, FFN_DIM), jnp.float32) * MODEL_DIM ** -0.5
    w_down = jax.random.normal(keys[4], (NUM_EXPERTS, FFN_DIM, MODEL_DIM), jnp.float32) * (2.0 * FFN_DIM ** -0.5)
    return {'tokens': tokens.astype(jnp.bfloat16), 'expert_ids': expert_ids, 'norm_gain': norm_gain.astype(jnp.bfloat16), 'router_w': router_w.astype(jnp.bfloat16), 'w_gate': w_gate.astype(jnp.bfloat16), 'w_up': w_up.astype(jnp.bfloat16), 'w_down': w_down.astype(jnp.bfloat16)}


def expert_ffn(operands):
    rows, gate_mat, up_mat, down_mat = operands
    gate_act = jnp.dot(rows, gate_mat, preferred_element_type=jnp.float32)
    up_act = jnp.dot(rows, up_mat, preferred_element_type=jnp.float32)
    hidden = (jax.nn.silu(gate_act) * up_act).astype(jnp.bfloat16)
    return jnp.dot(hidden, down_mat, preferred_element_type=jnp.float32).astype(jnp.bfloat16)


def reference(tokens, expert_ids, norm_gain, router_w, w_gate, w_up, w_down):
    tok_f32 = tokens.astype(jnp.float32)
    inv_rms = lax.rsqrt(jnp.mean(tok_f32 * tok_f32, axis=-1, keepdims=True) + NORM_EPS)
    normed = (tok_f32 * inv_rms * norm_gain.astype(jnp.float32)).astype(jnp.bfloat16)
    logits = jnp.dot(normed, router_w, preferred_element_type=jnp.float32)
    gates = jax.nn.softmax(jnp.take_along_axis(logits, expert_ids, axis=1), axis=-1)
    flat_ids = expert_ids.reshape(-1)
    onehot = (flat_ids[:, None] == jnp.arange(NUM_EXPERTS, dtype=jnp.int32)[None, :]).astype(jnp.int32)
    slot_ids = jnp.sum(jnp.cumsum(onehot, axis=0) * onehot, axis=1) - 1
    row_tok = jnp.arange(TOKENS * TOP_K, dtype=jnp.int32) // TOP_K
    src_rows = jnp.zeros((NUM_EXPERTS, EXPERT_CAP), jnp.int32).at[flat_ids, slot_ids].set(row_tok)
    buffers = normed[src_rows]
    expert_out = lax.map(expert_ffn, (buffers, w_gate, w_up, w_down))
    picked = expert_out[flat_ids, slot_ids].reshape(TOKENS, TOP_K, MODEL_DIM).astype(jnp.float32)
    mixed = jnp.sum(gates[:, :, None] * picked, axis=1)
    return (tok_f32 + mixed).astype(jnp.bfloat16)
```

```python
import functools

import jax
import jax.numpy as jnp
from jax import lax
from jax.experimental import pallas as pl
from jax.experimental.pallas import tpu as pltpu
from jax.sharding import PartitionSpec as P

NORM_EPS = 1e-5
CORES = 2
SLOTS = 12
VMEM_BYTES = 67_043_328
MESH = pl.DeviceIdType.MESH
PIECES = 4
CHUNK = 256
LAG_X = 1
LAG_Y = 4
LAG_O = 7


def split_bf16(val):
    hi = val.astype(jnp.bfloat16)
    rest = val - hi.astype(jnp.float32)
    mid = rest.astype(jnp.bfloat16)
    low = (rest - mid.astype(jnp.float32)).astype(jnp.bfloat16)
    return hi, mid, low


def moe_kernel(tok_hbm, ids_hbm, gain_hbm, wr_hbm, w1_hbm, w3_hbm, w2_hbm, out_ref,
               x_all, ids_all, gain, wr, wbuf, rows, slot_s, gate_s, comb, hid, ybuf, part,
               d_recv, x_send, kept, x_recv, y_recv,
               in_sem, w13_sem, w2_sem, xs_sem, xr_sem, is_sem, ir_sem, ds_sem, dr_sem):
    num_tok, dim = tok_hbm.shape
    top_k = ids_hbm.shape[0]
    num_exp = wr_hbm.shape[0]
    local_exp, kparts = w1_hbm.shape[:2]
    width = w1_hbm.shape[3]
    cap = rows.shape[1] // local_exp
    slots = local_exp * cap
    half_exp = wbuf.shape[1]
    num_chunk = dim // CHUNK
    per_pair = width // CHUNK

    ep = lax.axis_index('ep')
    tp = lax.axis_index('tp')
    core = ep % CORES
    chip = ep // CORES
    mate = {'ep': CORES * chip + 1 - core}
    across = {'ep': CORES * (1 - chip) + core}
    twin = {'tp': 1 - tp}
    b_mate = CORES * chip + 1 - core
    b_across = CORES * (1 - chip) + core
    b_diag = CORES * (1 - chip) + 1 - core

    def w13_copy(e, which):
        src = (w1_hbm, w3_hbm)[which]
        return pltpu.make_async_copy(
            src.at[e], wbuf.at[e % SLOTS, pl.ds(which * kparts, kparts)], w13_sem.at[e, which])

    def w2_copy(j, half):
        col = pl.multiple_of(j * CHUNK, CHUNK)
        sub = pl.multiple_of((j % per_pair) * CHUNK, CHUNK)
        return pltpu.make_async_copy(
            w2_hbm.at[pl.ds(half * half_exp, half_exp), :, pl.ds(col, CHUNK)],
            wbuf.at[SLOTS - num_chunk // per_pair * 2 + (j // per_pair) * 2 + half, :, :, pl.ds(sub, CHUNK)],
            w2_sem.at[j, half])

    own_x = pltpu.make_async_copy(tok_hbm, x_all.at[ep], in_sem.at[0])
    own_ids = pltpu.make_async_copy(ids_hbm, ids_all.at[ep], in_sem.at[1])
    get_wr = pltpu.make_async_copy(wr_hbm, wr, in_sem.at[2])
    get_gain = pltpu.make_async_copy(gain_hbm, gain, in_sem.at[3])
    for copy in (own_x, own_ids, get_gain, get_wr):
        copy.start()
    barrier = pltpu.get_barrier_semaphore()
    for peer in (mate, across, twin):
        pl.semaphore_signal(barrier, inc=1, device_id=peer, device_id_type=MESH)

    def start_w13(e, carry):
        w13_copy(e, 0).start(priority=1)
        w13_copy(e, 1).start(priority=1)
        return carry

    lax.fori_loop(0, SLOTS, start_w13, 0)

    piece = num_tok // PIECES

    def x_part(block, p):
        return x_all.at[block, pl.ds(p * piece, piece)]

    def remote(src, dst, ssem, rsem, peer):
        return pltpu.make_async_remote_copy(
            src_ref=src, dst_ref=dst, send_sem=ssem, recv_sem=rsem, device_id=peer, device_id_type=MESH)

    ids_mate = remote(ids_all.at[ep], ids_all.at[ep], is_sem.at[0], ir_sem.at[0], mate)
    ids_across = remote(ids_all.at[ep], ids_all.at[ep], is_sem.at[1], ir_sem.at[1], across)
    ids_diag = remote(ids_all.at[b_across], ids_all.at[b_across], is_sem.at[2], ir_sem.at[2], mate)
    x_mate = remote(x_all.at[ep], x_all.at[ep], xs_sem.at[2 * PIECES], xr_sem.at[2 * PIECES], mate)
    x_across = [remote(x_part(ep, p), x_part(ep, p), xs_sem.at[p], xr_sem.at[p], across)
                for p in range(PIECES)]
    x_diag = [remote(x_part(b_across, p), x_part(b_across, p), xs_sem.at[PIECES + p], xr_sem.at[PIECES + p], mate)
              for p in range(PIECES)]

    own_ids.wait()
    own_x.wait()
    pl.semaphore_wait(barrier, 3)
    ids_across.start()
    for copy in x_across:
        copy.start()
    ids_mate.start()
    x_mate.start()
    get_gain.wait()
    get_wr.wait()

    def take_block(block):
        tok = x_all[block].astype(jnp.float32)
        inv_rms = lax.rsqrt(jnp.mean(tok * tok, axis=-1, keepdims=True) + NORM_EPS)
        normed = (tok * inv_rms * gain[...].astype(jnp.float32)).astype(jnp.bfloat16)
        logits = lax.dot_general(wr[...], normed, (((1,), (1,)), ((), ())),
                                 preferred_element_type=jnp.float32)
        ids = ids_all[block]
        exp_iota = lax.broadcasted_iota(jnp.int32, (num_exp, num_tok), 0)
        member = exp_iota == ids[0:1, :]
        for k in range(1, top_k):
            member = member | (exp_iota == ids[k:k + 1, :])
        top = jnp.max(jnp.where(member, logits, -jnp.inf), axis=0, keepdims=True)
        weight = jnp.where(member, jnp.exp(jnp.where(member, logits - top, 0.0)), 0.0)
        gate_s[...] = weight / jnp.sum(weight, axis=0, keepdims=True)
        before = (lax.broadcasted_iota(jnp.int32, (num_tok, num_tok), 0)
                  < lax.broadcasted_iota(jnp.int32, (num_tok, num_tok), 1))
        rank = jnp.dot(jnp.where(member, 1.0, 0.0).astype(jnp.bfloat16),
                       jnp.where(before, 1.0, 0.0).astype(jnp.bfloat16), preferred_element_type=jnp.float32)
        slot_s[...] = jnp.where(member, rank, -1.0)
        first = pl.multiple_of(ep * local_exp, local_exp)
        slot_loc = slot_s[pl.ds(first, local_exp), :]
        gate_loc = gate_s[pl.ds(first, local_exp), :]
        slot_iota = lax.broadcasted_iota(jnp.int32, (cap, num_tok), 0).astype(jnp.float32)
        hits = [slot_iota == slot_loc[e:e + 1, :] for e in range(local_exp)]
        pick = jnp.concatenate([jnp.where(hit, 1.0, 0.0) for hit in hits], axis=0)
        rows[block] = jnp.dot(pick.astype(jnp.bfloat16), normed,
                              preferred_element_type=jnp.float32).astype(jnp.bfloat16)
        mix = jnp.concatenate([jnp.where(hits[e], gate_loc[e:e + 1, :], 0.0) for e in range(local_exp)], axis=0)
        comb[block] = jnp.concatenate(split_bf16(mix.T), axis=0)

    take_block(ep)
    ids_mate.wait_recv()
    x_mate.wait_recv()
    take_block(b_mate)
    ids_across.wait_recv()
    ids_diag.start()
    for p in range(PIECES):
        x_across[p].wait_recv()
        x_diag[p].start()
    take_block(b_across)
    ids_diag.wait_recv()
    for p in range(PIECES):
        x_diag[p].wait_recv()
    take_block(b_diag)

    blocks = rows.shape[0]

    def up_step(e, carry):
        w13_copy(e, 0).wait()
        w13_copy(e, 1).wait()
        first = pl.multiple_of(e * cap, cap)
        lhs = jnp.concatenate([rows[b, pl.ds(first, cap), :] for b in range(blocks)], axis=0)
        slot = e % SLOTS
        gate_act = jnp.dot(lhs, wbuf[slot, 0:kparts].reshape(dim, width), preferred_element_type=jnp.float32)
        up_act = jnp.dot(lhs, wbuf[slot, kparts:2 * kparts].reshape(dim, width), preferred_element_type=jnp.float32)
        hid[e] = (jax.nn.silu(gate_act) * up_act).astype(jnp.bfloat16)
        extra = local_exp - SLOTS

        @pl.when(e < extra)
        def _():
            start_w13(e + SLOTS, 0)

        @pl.when((e > extra) & (e < SLOTS) & ((e - extra) % 2 == 1))
        def _():
            for q in range(per_pair):
                for half in range(2):
                    w2_copy((e - extra) // 2 * per_pair + q, half).start(priority=1)

        return carry

    lax.fori_loop(0, local_exp, up_step, 0)

    def d_copy(j):
        return remote(part.at[j, 1 - core], d_recv.at[j], ds_sem.at[0, j], dr_sem.at[0, j], mate)

    def x_copy(j):
        return remote(x_send.at[j], x_recv.at[j], ds_sem.at[1, j], dr_sem.at[1, j], across)

    def y_copy(j):
        return remote(kept.at[j], y_recv.at[j], ds_sem.at[2, j], dr_sem.at[2, j], twin)

    def down_step(j, carry):
        @pl.when(j < num_chunk)
        def _():
            w2_copy(j, 0).wait()
            w2_copy(j, 1).wait()
            base = SLOTS - num_chunk // per_pair * 2 + (j // per_pair) * 2
            sub = pl.multiple_of((j % per_pair) * CHUNK, CHUNK)
            for e in range(local_exp):
                w2 = wbuf[base + e // half_exp, e % half_exp, :, pl.ds(sub, CHUNK)]
                y = jnp.dot(hid[e], w2, preferred_element_type=jnp.float32).astype(jnp.bfloat16)
                for b in range(blocks):
                    ybuf[b, e * cap:(e + 1) * cap, :] = y[b * cap:(b + 1) * cap, :]

            def mix_block(to_core, to_chip):
                block = CORES * to_chip + to_core
                three = jnp.dot(comb[block], ybuf[block], preferred_element_type=jnp.float32)
                part[j, to_core, to_chip] = (three[0:num_tok] + three[num_tok:2 * num_tok]) + three[2 * num_tok:]

            mix_block(1 - core, 0)
            mix_block(1 - core, 1)
            d_copy(j).start()
            mix_block(core, 0)
            mix_block(core, 1)

        @pl.when((j >= LAG_X) & (j < num_chunk + LAG_X))
        def _():
            i = j - LAG_X
            d_copy(i).wait_recv()
            x_send[i] = part[i, core, 1 - chip] + d_recv[i, 1 - chip]
            x_copy(i).start()
            kept[i] = part[i, core, chip] + d_recv[i, chip]

        @pl.when((j >= LAG_Y) & (j < num_chunk + LAG_Y))
        def _():
            i = j - LAG_Y
            x_copy(i).wait_recv()
            kept[i] = kept[i] + x_recv[i]
            y_copy(i).start()

        @pl.when(j >= LAG_O)
        def _():
            i = j - LAG_O
            y_copy(i).wait_recv()
            col = pl.multiple_of(i * CHUNK, CHUNK)
            tok = x_all[ep, :, pl.ds(col, CHUNK)].astype(jnp.float32)
            out_ref[:, pl.ds(col, CHUNK)] = (tok + (kept[i] + y_recv[i])).astype(out_ref.dtype)

        return carry

    lax.fori_loop(0, num_chunk + LAG_O, down_step, 0)

    for copy in (ids_mate, ids_across, ids_diag, x_mate, *x_across, *x_diag):
        copy.wait_send()

    def drain(j, carry):
        d_copy(j).wait_send()
        x_copy(j).wait_send()
        y_copy(j).wait_send()
        return carry

    lax.fori_loop(0, num_chunk, drain, 0)


def moe_call(ep_size, tokens, ids_t, gain, router_t, w_gate, w_up, w_down):
    num_tok, dim = tokens.shape
    top_k = ids_t.shape[0]
    num_exp = router_t.shape[0]
    local_exp, width, _ = w_down.shape
    cap = 2 * top_k * num_tok // num_exp
    kparts = dim // width
    half_exp = local_exp // 2
    chunks = dim // CHUNK
    w_gate = w_gate.reshape(local_exp, kparts, width, width)
    w_up = w_up.reshape(local_exp, kparts, width, width)
    bf16, f32 = jnp.bfloat16, jnp.float32
    vmem = pltpu.VMEM
    dma = pltpu.SemaphoreType.DMA
    any_spec = pl.BlockSpec(memory_space=pl.ANY)
    return pl.pallas_call(
        moe_kernel,
        out_shape=jax.ShapeDtypeStruct((num_tok, dim), tokens.dtype),
        in_specs=[any_spec] * 7,
        out_specs=pl.BlockSpec(memory_space=pltpu.VMEM),
        scratch_shapes=[
            vmem((ep_size, num_tok, dim), bf16),
            vmem((ep_size, top_k, num_tok), jnp.int32),
            vmem((1, dim), bf16),
            vmem((num_exp, dim), bf16),
            vmem((SLOTS, half_exp, width, width), bf16),
            vmem((ep_size, local_exp * cap, dim), bf16),
            vmem((num_exp, num_tok), f32),
            vmem((num_exp, num_tok), f32),
            vmem((ep_size, 3 * num_tok, local_exp * cap), bf16),
            vmem((local_exp, ep_size * cap, width), bf16),
            vmem((ep_size, local_exp * cap, CHUNK), bf16),
            vmem((chunks, CORES, ep_size // CORES, num_tok, CHUNK), f32),
            vmem((chunks, ep_size // CORES, num_tok, CHUNK), f32),
            vmem((chunks, num_tok, CHUNK), f32),
            vmem((chunks, num_tok, CHUNK), f32),
            vmem((chunks, num_tok, CHUNK), f32),
            vmem((chunks, num_tok, CHUNK), f32),
            dma((4,)), dma((local_exp, 2)), dma((chunks, 2)),
            dma((2 * PIECES + 1,)), dma((2 * PIECES + 1,)), dma((3,)), dma((3,)),
            dma((3, chunks)), dma((3, chunks)),
        ],
        compiler_params=pltpu.CompilerParams(
            collective_id=0, has_side_effects=True, vmem_limit_bytes=VMEM_BYTES),
        name='moe_block',
    )(tokens, ids_t, gain, router_t, w_gate, w_up, w_down)


def solution(mesh):
    ep_size = mesh.shape['ep']
    tok_spec = P(('dp', 'ep'), None)

    def local_block(tokens, expert_ids, norm_gain, router_w, w_gate, w_up, w_down):
        return moe_call(ep_size, tokens, expert_ids.T, norm_gain.reshape(1, -1), router_w.T, w_gate, w_up, w_down)

    return jax.shard_map(local_block, mesh=mesh, in_specs=(tok_spec, tok_spec, P(None), P(None, None), P('ep', None, 'tp'), P('ep', None, 'tp'), P('ep', 'tp', None)), out_specs=tok_spec, check_vma=False)
```

```python
import jax
import jax.numpy as jnp
from jax import lax
from jax.experimental import pallas as pl
from jax.experimental.pallas import tpu as pltpu
from jax.sharding import PartitionSpec as P

NORM_EPS = 1e-5
CORES = 2
SLOTS = 11
VMEM_BYTES = 63 * 2**20
MESH = pl.DeviceIdType.MESH
PIECE = 8
DIRECT = 6
CHUNK = 256
PARTS = 2
GROUP = 4
LAG_X = 1
LAG_Y = 4
LAG_O = 8


def split_bf16(val):
    hi = val.astype(jnp.bfloat16)
    rest = val - hi.astype(jnp.float32)
    mid = rest.astype(jnp.bfloat16)
    low = (rest - mid.astype(jnp.float32)).astype(jnp.bfloat16)
    return hi, mid, low


def moe_kernel(tok_hbm, ids_hbm, gain_hbm, wr_hbm, w1_hbm, w3_hbm, w2_hbm, out_ref,
               x_all, ids_all, gain, wr, wbuf, normed, rows, slot_s, gate_s, pick, comb, hid, ybuf, part,
               d_recv, x_send, kept, x_recv, y_recv,
               in_sem, w_sem, xa_rs, xt_rs, xd_rs, xm_rs, ir_sem, dr_sem, xr_sem, yr_sem, send_sem):
    num_tok, dim = tok_hbm.shape
    top_k = ids_hbm.shape[0]
    num_exp = wr_hbm.shape[0]
    local_exp, kparts = w1_hbm.shape[:2]
    width = w1_hbm.shape[3]
    blocks = rows.shape[0]
    cap = rows.shape[1] // local_exp
    half_exp = wbuf.shape[1]
    num_chunk = dim // CHUNK
    per_pair = width // CHUNK
    extra = local_exp - SLOTS
    scope = jax.named_scope

    ep = lax.axis_index('ep')
    tp = lax.axis_index('tp')
    core = ep % CORES
    chip = ep // CORES
    b_mate = CORES * chip + 1 - core
    b_across = CORES * (1 - chip) + core
    b_diag = CORES * (1 - chip) + 1 - core
    mate = {'ep': b_mate}
    across = {'ep': b_across}
    twin = {'tp': 1 - tp}

    def w13_copy(e, which):
        src = (w1_hbm, w3_hbm)[which]
        return pltpu.make_async_copy(
            src.at[e], wbuf.at[e % SLOTS, pl.ds(which * kparts, kparts)], w_sem.at[e % SLOTS])

    def w2_slot(j, half):
        return (extra + (j // per_pair) * 2 + half) % SLOTS

    def w2_copy(j, half):
        col = pl.multiple_of(j * CHUNK, CHUNK)
        sub = pl.multiple_of((j % per_pair) * CHUNK, CHUNK)
        return pltpu.make_async_copy(
            w2_hbm.at[pl.ds(half * half_exp, half_exp), :, pl.ds(col, CHUNK)],
            wbuf.at[w2_slot(j, half), :, :, pl.ds(sub, CHUNK)], w_sem.at[w2_slot(j, j % per_pair)])

    def w_wait(slot):
        pltpu.make_async_copy(wbuf.at[slot], wbuf.at[slot], w_sem.at[slot]).wait()

    own_x = pltpu.make_async_copy(tok_hbm, x_all.at[ep], in_sem.at[0])
    own_ids = pltpu.make_async_copy(ids_hbm, ids_all.at[ep], in_sem.at[1])
    get_wr = pltpu.make_async_copy(wr_hbm, wr, in_sem.at[2])
    get_gain = pltpu.make_async_copy(gain_hbm, gain, in_sem.at[3])
    for copy in (own_x, own_ids, get_gain, get_wr):
        copy.start()
    barrier = pltpu.get_barrier_semaphore()
    for peer in (mate, across, twin):
        pl.semaphore_signal(barrier, inc=1, device_id=peer, device_id_type=MESH)

    def start_w13(e, carry):
        w13_copy(e, 0).start(priority=1)
        w13_copy(e, 1).start(priority=1)
        return carry

    lax.fori_loop(0, SLOTS, start_w13, 0)

    def remote(src, dst, ssem, rsem, peer):
        return pltpu.make_async_remote_copy(
            src_ref=src, dst_ref=dst, send_sem=ssem, recv_sem=rsem, device_id=peer, device_id_type=MESH)

    pieces = num_tok // PIECE

    def x_part(block, k, side):
        first = pl.multiple_of((k + side * (pieces - 1 - 2 * k)) * PIECE, PIECE)
        return x_all.at[block, pl.ds(first, PIECE)]

    def same(ref, ssem, rsem, peer):
        return remote(ref, ref, ssem, rsem, peer)

    swapped = pieces - DIRECT
    ids_mate = same(ids_all.at[ep], send_sem.at[0], ir_sem.at[0], mate)
    ids_across = same(ids_all.at[ep], send_sem.at[0], ir_sem.at[1], across)
    ids_diag = same(ids_all.at[b_across], send_sem.at[0], ir_sem.at[2], mate)
    x_mate = same(x_all.at[ep], send_sem.at[1], xm_rs.at[0], mate)
    x_across = [same(x_part(ep, k, tp), send_sem.at[2], xa_rs.at[k], across) for k in range(DIRECT)]
    x_twin = [same(x_part(b_across, k, tp), send_sem.at[3], xt_rs.at[k], twin) for k in range(swapped)]
    x_diag = [same(x_part(b_across, k, tp), send_sem.at[4], xd_rs.at[0], mate) for k in range(pieces)]
    all_ids = same(ids_all.at[pl.ds(0, 3)], send_sem.at[0], ir_sem.at[0], mate)
    all_across = same(x_all.at[0, pl.ds(0, DIRECT * PIECE)], send_sem.at[2], xa_rs.at[0], across)
    all_twin = same(x_all.at[0, pl.ds(0, swapped * PIECE)], send_sem.at[3], xt_rs.at[0], twin)
    all_diag = same(x_all.at[b_diag], send_sem.at[4], xd_rs.at[0], mate)

    with scope('wait_own'):
        own_ids.wait()
        own_x.wait()
    with scope('wait_barrier'):
        pl.semaphore_wait(barrier, 3)
    ids_across.start()
    for copy in x_across:
        copy.start()
    ids_mate.start()
    x_mate.start()
    get_gain.wait()
    get_wr.wait()

    def route(block):
        ids = ids_all[block]
        exp_iota = lax.broadcasted_iota(jnp.int32, (num_exp, num_tok), 0)
        member = exp_iota == ids[0:1, :]
        for k in range(1, top_k):
            member = member | (exp_iota == ids[k:k + 1, :])
        before = (lax.broadcasted_iota(jnp.int32, (num_tok, num_tok), 0)
                  < lax.broadcasted_iota(jnp.int32, (num_tok, num_tok), 1))
        rank = jnp.dot(jnp.where(member, 1.0, 0.0).astype(jnp.bfloat16),
                       jnp.where(before, 1.0, 0.0).astype(jnp.bfloat16), preferred_element_type=jnp.float32)
        slot_s[block] = jnp.where(member, rank, -1.0)
        first = pl.multiple_of(ep * local_exp, local_exp)
        slot_loc = slot_s[block, pl.ds(first, local_exp), :]
        slot_iota = lax.broadcasted_iota(jnp.int32, (cap, num_tok), 0).astype(jnp.float32)
        pick[block] = jnp.concatenate(
            [jnp.where(slot_iota == slot_loc[e:e + 1, :], 1.0, 0.0) for e in range(local_exp)],
            axis=0).astype(jnp.bfloat16)

    def norm_rows(block):
        tok = x_all[block].astype(jnp.float32)
        inv_rms = lax.rsqrt(jnp.mean(tok * tok, axis=-1, keepdims=True) + NORM_EPS)
        scale = gain[...].astype(jnp.float32)
        scale = jnp.concatenate([scale[r:r + 1] for r in range(scale.shape[0])], axis=1)
        norm = (tok * inv_rms * scale).astype(jnp.bfloat16)
        normed[block] = norm

    def gather(block):
        rows[block] = jnp.dot(pick[block], normed[block], preferred_element_type=jnp.float32).astype(jnp.bfloat16)

    def gates(block):
        logits = lax.dot_general(wr[...], normed[block], (((1,), (1,)), ((), ())),
                                 preferred_element_type=jnp.float32)
        member = slot_s[block] >= 0.0
        top = jnp.max(jnp.where(member, logits, -jnp.inf), axis=0, keepdims=True)
        weight = jnp.where(member, jnp.exp(jnp.where(member, logits - top, 0.0)), 0.0)
        gate_s[...] = weight / jnp.sum(weight, axis=0, keepdims=True)
        first = pl.multiple_of(ep * local_exp, local_exp)
        gate_loc = gate_s[pl.ds(first, local_exp), :]
        spread = jnp.concatenate(
            [jnp.broadcast_to(gate_loc[e:e + 1, :], (cap, num_tok)) for e in range(local_exp)], axis=0)
        mix = jnp.where(pick[block].astype(jnp.float32) > 0.0, spread, 0.0)
        comb[block] = jnp.concatenate(split_bf16(mix.T), axis=0)

    with scope('own'):
        route(ep)
        norm_rows(ep)
        gather(ep)
    with scope('wait_mate'):
        ids_mate.wait_recv()
    with scope('mate'):
        route(b_mate)
        x_mate.wait_recv()
        norm_rows(b_mate)
        gather(b_mate)
        gates(ep)
        gates(b_mate)
    with scope('route_across'):
        ids_across.wait_recv()
        ids_diag.start()
        route(b_across)

    def relay(k):
        x_across[k].wait_recv()
        if k < swapped:
            x_twin[k].start()
        x_diag[k].start()

    def from_twin(k):
        x_twin[k].wait_recv()
        x_diag[pieces - 1 - k].start()

    with scope('relay'):
        for k in range(DIRECT - swapped):
            relay(k)
    with scope('route_diag'):
        ids_diag.wait_recv()
        route(b_diag)
    with scope('relay'):
        for k in range(DIRECT - swapped, DIRECT):
            from_twin(k - DIRECT + swapped)
            relay(k)
    with scope('norm_across'):
        norm_rows(b_across)
    with scope('wait_diag'):
        all_diag.wait_recv()
    with scope('gather_rest'):
        norm_rows(b_diag)
        gather(b_across)
        gather(b_diag)

    def up_one(e):
        first = pl.multiple_of(e * cap, cap)
        count = blocks * cap
        lhs = jnp.concatenate([rows[b % blocks, pl.ds(first, cap), :] for b in range(2 * blocks)], axis=0)
        slot = e % SLOTS
        gate_act = jnp.dot(lhs, wbuf[slot, 0:kparts].reshape(dim, width), preferred_element_type=jnp.float32)
        up_act = jnp.dot(lhs, wbuf[slot, kparts:2 * kparts].reshape(dim, width), preferred_element_type=jnp.float32)
        hid[e] = (jax.nn.silu(gate_act[0:count]) * up_act[0:count]).astype(jnp.bfloat16)

    def refill(e):
        @pl.when(e < extra)
        def _():
            start_w13(e + SLOTS, 0)

        @pl.when((e > extra) & (e < extra + 2 * num_chunk // per_pair) & ((e - extra) % 2 == 1))
        def _():
            for q in range(per_pair):
                for half in range(2):
                    w2_copy((e - extra) // 2 * per_pair + q, half).start(priority=1)

    def up_step(group):
        def step(i, carry):
            with scope('up_wait'):
                for u in range(group):
                    w_wait((i * group + u) % SLOTS)
            for u in range(group):
                up_one(i * group + u)
            for u in range(group):
                refill(i * group + u)
            return carry
        return step

    early = local_exp // 4 * 3
    lax.fori_loop(0, early // GROUP, up_step(GROUP), 0)
    with scope('gates_rest'):
        gates(b_across)
        gates(b_diag)
    lax.fori_loop(early, local_exp, up_step(1), 0)
    for copy in (all_ids, x_mate, all_across, all_twin, all_diag):
        copy.wait_send()

    def d_copy(j):
        return remote(part.at[j, 1 - core], d_recv.at[j], send_sem.at[5], dr_sem.at[j], mate)

    part_rows = num_tok // PARTS

    def x_copy(j, r):
        span = pl.ds(r * part_rows, part_rows)
        return remote(x_send.at[j, span], x_recv.at[j, span], send_sem.at[6], xr_sem.at[j, r], across)

    def y_copy(j, r):
        span = pl.ds(r * part_rows, part_rows)
        return remote(kept.at[j, span], y_recv.at[j, span], send_sem.at[7], yr_sem.at[j, r], twin)

    def down(j):
        with scope('down_wait'):
            w_wait(w2_slot(j, j % per_pair))
        sub = pl.multiple_of((j % per_pair) * CHUNK, CHUNK)
        for e in range(local_exp):
            w2 = wbuf[w2_slot(j, e // half_exp), e % half_exp, :, pl.ds(sub, CHUNK)]
            lhs = jnp.concatenate([hid[e], hid[e]], axis=0)
            y = jnp.dot(lhs, w2, preferred_element_type=jnp.float32).astype(jnp.bfloat16)
            for b in range(blocks):
                ybuf[b, e * cap:(e + 1) * cap, :] = y[b * cap:(b + 1) * cap, :]

        def mix_block(to_core, to_chip):
            block = CORES * to_chip + to_core
            three = jnp.dot(comb[block], ybuf[block], preferred_element_type=jnp.float32)
            part[j, to_core, to_chip] = (three[0:num_tok] + three[num_tok:2 * num_tok]) + three[2 * num_tok:]

        mix_block(1 - core, 0)
        mix_block(1 - core, 1)
        d_copy(j).start()
        mix_block(core, 0)
        mix_block(core, 1)

    def to_across(i):
        with scope('d_wait'):
            d_copy(i).wait_recv()
        for r in range(PARTS):
            span = pl.ds(r * part_rows, part_rows)
            x_send[i, span] = part[i, core, 1 - chip, span] + d_recv[i, 1 - chip, span]
            x_copy(i, r).start()
        kept[i] = part[i, core, chip] + d_recv[i, chip]

    def to_twin(i):
        for r in range(PARTS):
            with scope('x_wait'):
                x_copy(i, r).wait_recv()
            span = pl.ds(r * part_rows, part_rows)
            kept[i, span] = kept[i, span] + x_recv[i, span]
            y_copy(i, r).start()

    def finish(i):
        with scope('y_wait'):
            for r in range(PARTS):
                y_copy(i, r).wait_recv()
        col = pl.multiple_of(i * CHUNK, CHUNK)
        tok = x_all[ep, :, pl.ds(col, CHUNK)].astype(jnp.float32)
        out_ref[:, pl.ds(col, CHUNK)] = (tok + (kept[i] + y_recv[i])).astype(out_ref.dtype)

    def down_step(j, carry):
        @pl.when(j < num_chunk)
        def _():
            down(j)

        @pl.when((j >= LAG_X) & (j < num_chunk + LAG_X))
        def _():
            to_across(j - LAG_X)

        @pl.when((j >= LAG_Y) & (j < num_chunk + LAG_Y))
        def _():
            to_twin(j - LAG_Y)

        @pl.when(j >= LAG_O)
        def _():
            finish(j - LAG_O)

        return carry

    lax.fori_loop(0, num_chunk + LAG_O, down_step, 0)
    remote(d_recv, d_recv, send_sem.at[5], dr_sem.at[0], mate).wait_send()
    remote(x_send, x_recv, send_sem.at[6], xr_sem.at[0, 0], across).wait_send()
    remote(kept, y_recv, send_sem.at[7], yr_sem.at[0, 0], twin).wait_send()


def moe_call(ep_size, tokens, ids_t, gain, router_t, w_gate, w_up, w_down):
    num_tok, dim = tokens.shape
    top_k = ids_t.shape[0]
    num_exp = router_t.shape[0]
    local_exp, width, _ = w_down.shape
    cap = 2 * top_k * num_tok // num_exp
    kparts = dim // width
    half_exp = local_exp // 2
    chunks = dim // CHUNK
    pieces = num_tok // PIECE
    w_gate = w_gate.reshape(local_exp, kparts, width, width)
    w_up = w_up.reshape(local_exp, kparts, width, width)
    bf16, f32 = jnp.bfloat16, jnp.float32
    vmem = pltpu.VMEM
    dma = pltpu.SemaphoreType.DMA
    any_spec = pl.BlockSpec(memory_space=pl.ANY)
    return pl.pallas_call(
        moe_kernel,
        out_shape=pltpu.VMEM((num_tok, dim), tokens.dtype),
        in_specs=[any_spec] * 7,
        out_specs=pl.BlockSpec(memory_space=pltpu.VMEM),
        scratch_shapes=[
            vmem((ep_size, num_tok, dim), bf16),
            vmem((ep_size, top_k, num_tok), jnp.int32),
            vmem(gain.shape, bf16),
            vmem((num_exp, dim), bf16),
            vmem((SLOTS, half_exp, width, width), bf16),
            vmem((ep_size, num_tok, dim), bf16),
            vmem((ep_size, local_exp * cap, dim), bf16),
            vmem((ep_size, num_exp, num_tok), f32),
            vmem((num_exp, num_tok), f32),
            vmem((ep_size, local_exp * cap, num_tok), bf16),
            vmem((ep_size, 3 * num_tok, local_exp * cap), bf16),
            vmem((local_exp, ep_size * cap, width), bf16),
            vmem((ep_size, local_exp * cap, CHUNK), bf16),
            vmem((chunks, CORES, ep_size // CORES, num_tok, CHUNK), f32),
            vmem((chunks, ep_size // CORES, num_tok, CHUNK), f32),
            vmem((chunks, num_tok, CHUNK), f32),
            vmem((chunks, num_tok, CHUNK), f32),
            vmem((chunks, num_tok, CHUNK), f32),
            vmem((chunks, num_tok, CHUNK), f32),
            dma((4,)), dma((SLOTS,)), dma((DIRECT,)), dma((pieces - DIRECT,)), dma((1,)), dma((1,)), dma((3,)),
            dma((chunks,)), dma((chunks, PARTS)), dma((chunks, PARTS)), dma((8,)),
        ],
        compiler_params=pltpu.CompilerParams(
            collective_id=0, has_side_effects=True, vmem_limit_bytes=VMEM_BYTES),
        name='moe_block',
    )(tokens, ids_t, gain, router_t, w_gate, w_up, w_down)


def solution(mesh):
    ep_size = mesh.shape['ep']
    tok_spec = P(('dp', 'ep'), None)

    def local_block(tokens, expert_ids, norm_gain, router_w, w_gate, w_up, w_down):
        return moe_call(ep_size, tokens, expert_ids.T, norm_gain.reshape(-1, 128), router_w.T, w_gate, w_up, w_down)

    return jax.shard_map(local_block, mesh=mesh, in_specs=(tok_spec, tok_spec, P(None), P(None, None), P('ep', None, 'tp'), P('ep', None, 'tp'), P('ep', 'tp', None)), out_specs=tok_spec, check_vma=False)
```

```python
import functools

import jax
import jax.numpy as jnp
from jax import lax
from jax.experimental import pallas as pl
from jax.experimental.pallas import tpu as pltpu
from jax.sharding import PartitionSpec as P

NORM_EPS = 1e-5
CORES = 2
SLOTS = 11
VMEM_BYTES = 63 * 2**20
MESH = pl.DeviceIdType.MESH
PIECE = 8
DIRECT = 6
CHUNK = 256
PARTS = 2
GROUP = 4
LAG_X = 1
LAG_Y = 4
LAG_O = 8


def split_bf16(val):
    hi = val.astype(jnp.bfloat16)
    rest = val - hi.astype(jnp.float32)
    mid = rest.astype(jnp.bfloat16)
    low = (rest - mid.astype(jnp.float32)).astype(jnp.bfloat16)
    return hi, mid, low


def moe_kernel(tok_hbm, ids_hbm, gain_hbm, wr_hbm, w1_hbm, w3_hbm, w2_hbm, out_ref,
               x_all, ids_all, gain, wr, wbuf, normed, rows, slot_s, gate_s, pick, comb, hid, ybuf, part,
               d_recv, x_send, kept, x_recv, y_recv,
               in_sem, w_sem, xa_rs, xt_rs, xd_rs, xm_rs, ir_sem, dr_sem, xr_sem, yr_sem, send_sem):
    num_tok, dim = tok_hbm.shape
    top_k = ids_hbm.shape[0]
    num_exp = wr_hbm.shape[0]
    local_exp, kparts = w1_hbm.shape[:2]
    width = w1_hbm.shape[3]
    blocks = rows.shape[0]
    cap = rows.shape[1] // local_exp
    half_exp = wbuf.shape[1]
    num_chunk = dim // CHUNK
    per_pair = width // CHUNK
    extra = local_exp - SLOTS
    scope = jax.named_scope

    ep = lax.axis_index('ep')
    tp = lax.axis_index('tp')
    core = ep % CORES
    chip = ep // CORES
    b_mate = CORES * chip + 1 - core
    b_across = CORES * (1 - chip) + core
    b_diag = CORES * (1 - chip) + 1 - core
    mate = {'ep': b_mate}
    across = {'ep': b_across}
    twin = {'tp': 1 - tp}

    def w13_copy(e, which):
        src = (w1_hbm, w3_hbm)[which]
        return pltpu.make_async_copy(
            src.at[e], wbuf.at[e % SLOTS, pl.ds(which * kparts, kparts)], w_sem.at[e % SLOTS])

    def w2_slot(j, half):
        return (extra + (j // per_pair) * 2 + half) % SLOTS

    def w2_copy(j, half):
        col = pl.multiple_of(j * CHUNK, CHUNK)
        sub = pl.multiple_of((j % per_pair) * CHUNK, CHUNK)
        return pltpu.make_async_copy(
            w2_hbm.at[pl.ds(half * half_exp, half_exp), :, pl.ds(col, CHUNK)],
            wbuf.at[w2_slot(j, half), :, :, pl.ds(sub, CHUNK)], w_sem.at[w2_slot(j, j % per_pair)])

    def w_wait(slot):
        pltpu.make_async_copy(wbuf.at[slot], wbuf.at[slot], w_sem.at[slot]).wait()

    own_x = pltpu.make_async_copy(tok_hbm, x_all.at[ep], in_sem.at[0])
    own_ids = pltpu.make_async_copy(ids_hbm, ids_all.at[ep], in_sem.at[1])
    get_wr = pltpu.make_async_copy(wr_hbm, wr, in_sem.at[2])
    get_gain = pltpu.make_async_copy(gain_hbm, gain, in_sem.at[3])
    for copy in (own_x, own_ids, get_gain, get_wr):
        copy.start()
    barrier = pltpu.get_barrier_semaphore()
    for peer in (mate, across, twin):
        pl.semaphore_signal(barrier, inc=1, device_id=peer, device_id_type=MESH)

    def start_w13(e, carry):
        w13_copy(e, 0).start(priority=1)
        w13_copy(e, 1).start(priority=1)
        return carry

    lax.fori_loop(0, SLOTS, start_w13, 0)

    def remote(src, dst, ssem, rsem, peer):
        return pltpu.make_async_remote_copy(
            src_ref=src, dst_ref=dst, send_sem=ssem, recv_sem=rsem, device_id=peer, device_id_type=MESH)

    pieces = num_tok // PIECE

    def x_part(block, k, side):
        first = pl.multiple_of((k + side * (pieces - 1 - 2 * k)) * PIECE, PIECE)
        return x_all.at[block, pl.ds(first, PIECE)]

    def same(ref, ssem, rsem, peer):
        return remote(ref, ref, ssem, rsem, peer)

    swapped = pieces - DIRECT
    ids_mate = same(ids_all.at[ep], send_sem.at[0], ir_sem.at[0], mate)
    ids_across = same(ids_all.at[ep], send_sem.at[0], ir_sem.at[1], across)
    ids_diag = same(ids_all.at[b_across], send_sem.at[0], ir_sem.at[2], mate)
    x_mate = same(x_all.at[ep], send_sem.at[1], xm_rs.at[0], mate)
    x_across = [same(x_part(ep, k, tp), send_sem.at[2], xa_rs.at[k], across) for k in range(DIRECT)]
    x_twin = [same(x_part(b_across, k, tp), send_sem.at[3], xt_rs.at[k], twin) for k in range(swapped)]
    x_diag = [same(x_part(b_across, k, tp), send_sem.at[4], xd_rs.at[0], mate) for k in range(pieces)]
    all_ids = same(ids_all.at[pl.ds(0, 3)], send_sem.at[0], ir_sem.at[0], mate)
    all_across = same(x_all.at[0, pl.ds(0, DIRECT * PIECE)], send_sem.at[2], xa_rs.at[0], across)
    all_twin = same(x_all.at[0, pl.ds(0, swapped * PIECE)], send_sem.at[3], xt_rs.at[0], twin)
    all_diag = same(x_all.at[b_diag], send_sem.at[4], xd_rs.at[0], mate)

    with scope('wait_own'):
        own_ids.wait()
        own_x.wait()
    with scope('wait_barrier'):
        pl.semaphore_wait(barrier, 3)
    ids_across.start()
    for copy in x_across:
        copy.start()
    ids_mate.start()
    x_mate.start()
    get_gain.wait()
    get_wr.wait()

    def route(block):
        ids = ids_all[block]
        exp_iota = lax.broadcasted_iota(jnp.int32, (num_exp, num_tok), 0)
        member = exp_iota == ids[0:1, :]
        for k in range(1, top_k):
            member = member | (exp_iota == ids[k:k + 1, :])
        before = (lax.broadcasted_iota(jnp.int32, (num_tok, num_tok), 0)
                  < lax.broadcasted_iota(jnp.int32, (num_tok, num_tok), 1))
        rank = jnp.dot(jnp.where(member, 1.0, 0.0).astype(jnp.bfloat16),
                       jnp.where(before, 1.0, 0.0).astype(jnp.bfloat16), preferred_element_type=jnp.float32)
        slot_s[block] = jnp.where(member, rank, -1.0)
        first = pl.multiple_of(ep * local_exp, local_exp)
        slot_loc = slot_s[block, pl.ds(first, local_exp), :]
        slot_iota = lax.broadcasted_iota(jnp.int32, (cap, num_tok), 0).astype(jnp.float32)
        pick[block] = jnp.concatenate(
            [jnp.where(slot_iota == slot_loc[e:e + 1, :], 1.0, 0.0) for e in range(local_exp)],
            axis=0).astype(jnp.bfloat16)

    def norm_rows(block):
        tok = x_all[block].astype(jnp.float32)
        inv_rms = lax.rsqrt(jnp.mean(tok * tok, axis=-1, keepdims=True) + NORM_EPS)
        scale = gain[...].astype(jnp.float32)
        scale = jnp.concatenate([scale[r:r + 1] for r in range(scale.shape[0])], axis=1)
        norm = (tok * inv_rms * scale).astype(jnp.bfloat16)
        normed[block] = norm

    def gather(block):
        rows[block] = jnp.dot(pick[block], normed[block], preferred_element_type=jnp.float32).astype(jnp.bfloat16)

    def gates(block):
        logits = lax.dot_general(wr[...], normed[block], (((1,), (1,)), ((), ())),
                                 preferred_element_type=jnp.float32)
        member = slot_s[block] >= 0.0
        top = jnp.max(jnp.where(member, logits, -jnp.inf), axis=0, keepdims=True)
        weight = jnp.where(member, jnp.exp(jnp.where(member, logits - top, 0.0)), 0.0)
        gate_s[...] = weight / jnp.sum(weight, axis=0, keepdims=True)
        first = pl.multiple_of(ep * local_exp, local_exp)
        gate_loc = gate_s[pl.ds(first, local_exp), :]
        spread = jnp.concatenate(
            [jnp.broadcast_to(gate_loc[e:e + 1, :], (cap, num_tok)) for e in range(local_exp)], axis=0)
        mix = jnp.where(pick[block].astype(jnp.float32) > 0.0, spread, 0.0)
        comb[block] = jnp.concatenate(split_bf16(mix.T), axis=0)

    with scope('own'):
        route(ep)
        norm_rows(ep)
        gather(ep)
    with scope('wait_mate'):
        ids_mate.wait_recv()
    with scope('mate'):
        route(b_mate)
        x_mate.wait_recv()
        norm_rows(b_mate)
        gather(b_mate)
        gates(ep)
        gates(b_mate)
    with scope('route_across'):
        ids_across.wait_recv()
        ids_diag.start()
        route(b_across)

    def relay(k):
        x_across[k].wait_recv()
        if k < swapped:
            x_twin[k].start()
        x_diag[k].start()

    def from_twin(k):
        x_twin[k].wait_recv()
        x_diag[pieces - 1 - k].start()

    with scope('relay'):
        for k in range(DIRECT - swapped):
            relay(k)
    with scope('route_diag'):
        ids_diag.wait_recv()
        route(b_diag)
    with scope('relay'):
        for k in range(DIRECT - swapped, DIRECT):
            from_twin(k - DIRECT + swapped)
            relay(k)
    with scope('norm_across'):
        norm_rows(b_across)
    with scope('wait_diag'):
        all_diag.wait_recv()
    with scope('gather_rest'):
        norm_rows(b_diag)
        gather(b_across)
        gather(b_diag)

    def up_one(e):
        first = pl.multiple_of(e * cap, cap)
        count = blocks * cap
        lhs = jnp.concatenate([rows[b % blocks, pl.ds(first, cap), :] for b in range(2 * blocks)], axis=0)
        slot = e % SLOTS
        gate_act = jnp.dot(lhs, wbuf[slot, 0:kparts].reshape(dim, width), preferred_element_type=jnp.float32)
        up_act = jnp.dot(lhs, wbuf[slot, kparts:2 * kparts].reshape(dim, width), preferred_element_type=jnp.float32)
        hid[e] = (jax.nn.silu(gate_act[0:count]) * up_act[0:count]).astype(jnp.bfloat16)

    def refill(e):
        @pl.when(e < extra)
        def _():
            start_w13(e + SLOTS, 0)

        @pl.when((e > extra) & (e < extra + 2 * num_chunk // per_pair) & ((e - extra) % 2 == 1))
        def _():
            for q in range(per_pair):
                for half in range(2):
                    w2_copy((e - extra) // 2 * per_pair + q, half).start(priority=1)

    def up_step(group):
        def step(i, carry):
            with scope('up_wait'):
                for u in range(group):
                    w_wait((i * group + u) % SLOTS)
            for u in range(group):
                up_one(i * group + u)
            for u in range(group):
                refill(i * group + u)
            return carry
        return step

    fours, pairs = local_exp // 2, local_exp // 4 * 3
    lax.fori_loop(0, fours // 4, up_step(4), 0)
    lax.fori_loop(fours // 2, pairs // 2, up_step(2), 0)
    with scope('gates_rest'):
        gates(b_across)
        gates(b_diag)
    lax.fori_loop(pairs, local_exp, up_step(1), 0)
    for copy in (all_ids, x_mate, all_across, all_twin, all_diag):
        copy.wait_send()

    def d_copy(j):
        return remote(part.at[j, 1 - core], d_recv.at[j], send_sem.at[5], dr_sem.at[j], mate)

    part_rows = num_tok // PARTS

    def x_copy(j, r):
        span = pl.ds(r * part_rows, part_rows)
        return remote(x_send.at[j, span], x_recv.at[j, span], send_sem.at[6], xr_sem.at[j, r], across)

    def y_copy(j, r):
        span = pl.ds(r * part_rows, part_rows)
        return remote(kept.at[j, span], y_recv.at[j, span], send_sem.at[7], yr_sem.at[j], twin)

    def down(j):
        with scope('down_wait'):
            w_wait(w2_slot(j, j % per_pair))
        sub = pl.multiple_of((j % per_pair) * CHUNK, CHUNK)
        for e in range(local_exp):
            w2 = wbuf[w2_slot(j, e // half_exp), e % half_exp, :, pl.ds(sub, CHUNK)]
            lhs = jnp.concatenate([hid[e], hid[e]], axis=0)
            y = jnp.dot(lhs, w2, preferred_element_type=jnp.float32).astype(jnp.bfloat16)
            for b in range(blocks):
                ybuf[b, e * cap:(e + 1) * cap, :] = y[b * cap:(b + 1) * cap, :]

        def mix_block(to_core, to_chip):
            block = CORES * to_chip + to_core
            three = jnp.dot(comb[block], ybuf[block], preferred_element_type=jnp.float32)
            part[j, to_core, to_chip] = (three[0:num_tok] + three[num_tok:2 * num_tok]) + three[2 * num_tok:]

        mix_block(1 - core, 0)
        mix_block(1 - core, 1)
        d_copy(j).start()
        mix_block(core, 0)
        mix_block(core, 1)

    def to_across(i):
        with scope('d_wait'):
            d_copy(i).wait_recv()
        for r in range(PARTS):
            span = pl.ds(r * part_rows, part_rows)
            x_send[i, span] = part[i, core, 1 - chip, span] + d_recv[i, 1 - chip, span]
            x_copy(i, r).start()
        kept[i] = part[i, core, chip] + d_recv[i, chip]

    def to_twin(i):
        for r in range(PARTS):
            with scope('x_wait'):
                x_copy(i, r).wait_recv()
            span = pl.ds(r * part_rows, part_rows)
            kept[i, span] = kept[i, span] + x_recv[i, span]
            y_copy(i, r).start()

    def finish(i):
        with scope('y_wait'):
            remote(kept.at[i], y_recv.at[i], send_sem.at[7], yr_sem.at[i], twin).wait_recv()
        col = pl.multiple_of(i * CHUNK, CHUNK)
        tok = x_all[ep, :, pl.ds(col, CHUNK)].astype(jnp.float32)
        out_ref[:, pl.ds(col, CHUNK)] = (tok + (kept[i] + y_recv[i])).astype(out_ref.dtype)

    def down_step(j, carry):
        @pl.when(j < num_chunk)
        def _():
            down(j)

        @pl.when((j >= LAG_X) & (j < num_chunk + LAG_X))
        def _():
            to_across(j - LAG_X)

        @pl.when((j >= LAG_Y) & (j < num_chunk + LAG_Y))
        def _():
            to_twin(j - LAG_Y)

        @pl.when(j >= LAG_O)
        def _():
            finish(j - LAG_O)

        return carry

    lax.fori_loop(0, num_chunk + LAG_O, down_step, 0)
    remote(d_recv, d_recv, send_sem.at[5], dr_sem.at[0], mate).wait_send()
    remote(x_send, x_recv, send_sem.at[6], xr_sem.at[0, 0], across).wait_send()
    remote(kept, y_recv, send_sem.at[7], yr_sem.at[0], twin).wait_send()


def scoped_kernel(sems, *refs):
    pl.run_scoped(lambda *held: moe_kernel(*refs, *held), *sems)


def moe_call(ep_size, tokens, ids_t, gain, router_t, w_gate, w_up, w_down):
    num_tok, dim = tokens.shape
    top_k = ids_t.shape[0]
    num_exp = router_t.shape[0]
    local_exp, width, _ = w_down.shape
    cap = 2 * top_k * num_tok // num_exp
    kparts = dim // width
    half_exp = local_exp // 2
    chunks = dim // CHUNK
    pieces = num_tok // PIECE
    w_gate = w_gate.reshape(local_exp, kparts, width, width)
    w_up = w_up.reshape(local_exp, kparts, width, width)
    bf16, f32 = jnp.bfloat16, jnp.float32
    vmem = pltpu.VMEM
    dma = pltpu.SemaphoreType.DMA
    any_spec = pl.BlockSpec(memory_space=pl.ANY)
    sems = (
        dma((4,)), dma((SLOTS,)), dma((DIRECT,)), dma((pieces - DIRECT,)), dma((1,)), dma((1,)), dma((3,)),
        dma((chunks,)), dma((chunks, PARTS)), dma((chunks,)), dma((8,)),
    )
    return pl.pallas_call(
        functools.partial(scoped_kernel, sems),
        out_shape=pltpu.VMEM((num_tok, dim), tokens.dtype),
        in_specs=[any_spec] * 7,
        out_specs=pl.BlockSpec(memory_space=pltpu.VMEM),
        scratch_shapes=[
            vmem((ep_size, num_tok, dim), bf16),
            vmem((ep_size, top_k, num_tok), jnp.int32),
            vmem(gain.shape, bf16),
            vmem((num_exp, dim), bf16),
            vmem((SLOTS, half_exp, width, width), bf16),
            vmem((ep_size, num_tok, dim), bf16),
            vmem((ep_size, local_exp * cap, dim), bf16),
            vmem((ep_size, num_exp, num_tok), f32),
            vmem((num_exp, num_tok), f32),
            vmem((ep_size, local_exp * cap, num_tok), bf16),
            vmem((ep_size, 3 * num_tok, local_exp * cap), bf16),
            vmem((local_exp, ep_size * cap, width), bf16),
            vmem((ep_size, local_exp * cap, CHUNK), bf16),
            vmem((chunks, CORES, ep_size // CORES, num_tok, CHUNK), f32),
            vmem((chunks, ep_size // CORES, num_tok, CHUNK), f32),
            vmem((chunks, num_tok, CHUNK), f32),
            vmem((chunks, num_tok, CHUNK), f32),
            vmem((chunks, num_tok, CHUNK), f32),
            vmem((chunks, num_tok, CHUNK), f32),
        ],
        compiler_params=pltpu.CompilerParams(
            collective_id=0, has_side_effects=True, vmem_limit_bytes=VMEM_BYTES),
        name='moe_block',
    )(tokens, ids_t, gain, router_t, w_gate, w_up, w_down)


def solution(mesh):
    ep_size = mesh.shape['ep']
    tok_spec = P(('dp', 'ep'), None)

    def local_block(tokens, expert_ids, norm_gain, router_w, w_gate, w_up, w_down):
        return moe_call(ep_size, tokens, expert_ids.T, norm_gain.reshape(-1, 128), router_w.T, w_gate, w_up, w_down)

    return jax.shard_map(local_block, mesh=mesh, in_specs=(tok_spec, tok_spec, P(None), P(None, None), P('ep', None, 'tp'), P('ep', None, 'tp'), P('ep', 'tp', None)), out_specs=tok_spec, check_vma=False)
```

```python
import functools

import jax
import jax.numpy as jnp
from jax import lax
from jax.experimental import pallas as pl
from jax.experimental.pallas import tpu as pltpu
from jax.sharding import PartitionSpec as P

NORM_EPS = 1e-5
CORES = 2
SLOTS = 11
VMEM_BYTES = 63 * 2**20
MESH = pl.DeviceIdType.MESH
PIECE = 8
DIRECT = 6
CHUNK = 256
PARTS = 4
GROUP = 4
LAG_X = 1
LAG_Y = 4
LAG_O = 8


def split_bf16(val):
    hi = val.astype(jnp.bfloat16)
    rest = val - hi.astype(jnp.float32)
    mid = rest.astype(jnp.bfloat16)
    low = (rest - mid.astype(jnp.float32)).astype(jnp.bfloat16)
    return hi, mid, low


def moe_kernel(tok_hbm, ids_hbm, gain_hbm, wr_hbm, w1_hbm, w3_hbm, w2_hbm, out_ref,
               x_all, ids_all, gain, wr, wbuf, normed, rows, slot_s, gate_s, pick, comb, hid, ybuf, part,
               d_recv, x_send, kept, x_recv, y_recv,
               in_sem, w_sem, xa_rs, xt_rs, xd_rs, xm_rs, ir_sem, dr_sem, xr_sem, yr_sem, send_sem):
    num_tok, dim = tok_hbm.shape
    top_k = ids_hbm.shape[0]
    num_exp = wr_hbm.shape[0]
    local_exp, kparts = w1_hbm.shape[:2]
    width = w1_hbm.shape[3]
    blocks = rows.shape[0]
    cap = rows.shape[1] // local_exp
    half_exp = wbuf.shape[1]
    num_chunk = dim // CHUNK
    per_pair = width // CHUNK
    extra = local_exp - SLOTS
    scope = jax.named_scope

    ep = lax.axis_index('ep')
    tp = lax.axis_index('tp')
    core = ep % CORES
    chip = ep // CORES
    b_mate = CORES * chip + 1 - core
    b_across = CORES * (1 - chip) + core
    b_diag = CORES * (1 - chip) + 1 - core
    mate = {'ep': b_mate}
    across = {'ep': b_across}
    twin = {'tp': 1 - tp}

    def w13_copy(e, which):
        src = (w1_hbm, w3_hbm)[which]
        return pltpu.make_async_copy(
            src.at[e], wbuf.at[e % SLOTS, pl.ds(which * kparts, kparts)], w_sem.at[e % SLOTS])

    def w2_slot(j, half):
        return (extra + (j // per_pair) * 2 + half) % SLOTS

    def w2_copy(j, half):
        col = pl.multiple_of(j * CHUNK, CHUNK)
        sub = pl.multiple_of((j % per_pair) * CHUNK, CHUNK)
        return pltpu.make_async_copy(
            w2_hbm.at[pl.ds(half * half_exp, half_exp), :, pl.ds(col, CHUNK)],
            wbuf.at[w2_slot(j, half), :, :, pl.ds(sub, CHUNK)], w_sem.at[w2_slot(j, j % per_pair)])

    def w_wait(slot):
        pltpu.make_async_copy(wbuf.at[slot], wbuf.at[slot], w_sem.at[slot]).wait()

    own_x = pltpu.make_async_copy(tok_hbm, x_all.at[ep], in_sem.at[0])
    own_ids = pltpu.make_async_copy(ids_hbm, ids_all.at[ep], in_sem.at[1])
    get_wr = pltpu.make_async_copy(wr_hbm, wr, in_sem.at[2])
    get_gain = pltpu.make_async_copy(gain_hbm, gain, in_sem.at[3])
    for copy in (own_x, own_ids, get_gain, get_wr):
        copy.start()
    barrier = pltpu.get_barrier_semaphore()
    for peer in (mate, across, twin):
        pl.semaphore_signal(barrier, inc=1, device_id=peer, device_id_type=MESH)

    def start_w13(e, carry):
        w13_copy(e, 0).start(priority=1)
        w13_copy(e, 1).start(priority=1)
        return carry

    lax.fori_loop(0, SLOTS, start_w13, 0)

    def remote(src, dst, ssem, rsem, peer):
        return pltpu.make_async_remote_copy(
            src_ref=src, dst_ref=dst, send_sem=ssem, recv_sem=rsem, device_id=peer, device_id_type=MESH)

    pieces = num_tok // PIECE

    def x_part(block, k, side):
        first = pl.multiple_of((k + side * (pieces - 1 - 2 * k)) * PIECE, PIECE)
        return x_all.at[block, pl.ds(first, PIECE)]

    def same(ref, ssem, rsem, peer):
        return remote(ref, ref, ssem, rsem, peer)

    swapped = pieces - DIRECT
    ids_mate = same(ids_all.at[ep], send_sem.at[0], ir_sem.at[0], mate)
    ids_across = same(ids_all.at[ep], send_sem.at[0], ir_sem.at[1], across)
    ids_diag = same(ids_all.at[b_across], send_sem.at[0], ir_sem.at[2], mate)
    x_mate = same(x_all.at[ep], send_sem.at[1], xm_rs.at[0], mate)
    x_across = [same(x_part(ep, k, tp), send_sem.at[2], xa_rs.at[k], across) for k in range(DIRECT)]
    x_twin = [same(x_part(b_across, k, tp), send_sem.at[3], xt_rs.at[k], twin) for k in range(swapped)]
    x_diag = [same(x_part(b_across, k, tp), send_sem.at[4], xd_rs.at[0], mate) for k in range(pieces)]
    all_ids = same(ids_all.at[pl.ds(0, 3)], send_sem.at[0], ir_sem.at[0], mate)
    all_across = same(x_all.at[0, pl.ds(0, DIRECT * PIECE)], send_sem.at[2], xa_rs.at[0], across)
    all_twin = same(x_all.at[0, pl.ds(0, swapped * PIECE)], send_sem.at[3], xt_rs.at[0], twin)
    all_diag = same(x_all.at[b_diag], send_sem.at[4], xd_rs.at[0], mate)

    with scope('wait_own'):
        own_ids.wait()
        own_x.wait()
    with scope('wait_barrier'):
        pl.semaphore_wait(barrier, 3)
    ids_across.start()
    for copy in x_across:
        copy.start()
    ids_mate.start()
    x_mate.start()
    get_gain.wait()
    get_wr.wait()

    def route(block):
        ids = ids_all[block]
        exp_iota = lax.broadcasted_iota(jnp.int32, (num_exp, num_tok), 0)
        member = exp_iota == ids[0:1, :]
        for k in range(1, top_k):
            member = member | (exp_iota == ids[k:k + 1, :])
        before = (lax.broadcasted_iota(jnp.int32, (num_tok, num_tok), 0)
                  < lax.broadcasted_iota(jnp.int32, (num_tok, num_tok), 1))
        rank = jnp.dot(jnp.where(member, 1.0, 0.0).astype(jnp.bfloat16),
                       jnp.where(before, 1.0, 0.0).astype(jnp.bfloat16), preferred_element_type=jnp.float32)
        slot_s[block] = jnp.where(member, rank, -1.0)
        first = pl.multiple_of(ep * local_exp, local_exp)
        slot_loc = slot_s[block, pl.ds(first, local_exp), :]
        slot_iota = lax.broadcasted_iota(jnp.int32, (cap, num_tok), 0).astype(jnp.float32)
        pick[block] = jnp.concatenate(
            [jnp.where(slot_iota == slot_loc[e:e + 1, :], 1.0, 0.0) for e in range(local_exp)],
            axis=0).astype(jnp.bfloat16)

    def norm_rows(block):
        tok = x_all[block].astype(jnp.float32)
        inv_rms = lax.rsqrt(jnp.mean(tok * tok, axis=-1, keepdims=True) + NORM_EPS)
        scale = gain[...].astype(jnp.float32)
        scale = jnp.concatenate([scale[r:r + 1] for r in range(scale.shape[0])], axis=1)
        norm = (tok * inv_rms * scale).astype(jnp.bfloat16)
        normed[block] = norm

    def gather(block):
        rows[block] = jnp.dot(pick[block], normed[block], preferred_element_type=jnp.float32).astype(jnp.bfloat16)

    def gates(block):
        logits = lax.dot_general(wr[...], normed[block], (((1,), (1,)), ((), ())),
                                 preferred_element_type=jnp.float32)
        member = slot_s[block] >= 0.0
        top = jnp.max(jnp.where(member, logits, -jnp.inf), axis=0, keepdims=True)
        weight = jnp.where(member, jnp.exp(jnp.where(member, logits - top, 0.0)), 0.0)
        gate_s[...] = weight / jnp.sum(weight, axis=0, keepdims=True)
        first = pl.multiple_of(ep * local_exp, local_exp)
        gate_loc = gate_s[pl.ds(first, local_exp), :]
        spread = jnp.concatenate(
            [jnp.broadcast_to(gate_loc[e:e + 1, :], (cap, num_tok)) for e in range(local_exp)], axis=0)
        mix = jnp.where(pick[block].astype(jnp.float32) > 0.0, spread, 0.0)
        comb[block] = jnp.concatenate(split_bf16(mix.T), axis=0)

    with scope('own'):
        route(ep)
        norm_rows(ep)
        gather(ep)
    with scope('wait_mate'):
        ids_mate.wait_recv()
    with scope('mate'):
        route(b_mate)
        x_mate.wait_recv()
        norm_rows(b_mate)
        gather(b_mate)
        gates(ep)
        gates(b_mate)
    with scope('route_across'):
        ids_across.wait_recv()
        ids_diag.start()
        route(b_across)

    def relay(k):
        x_across[k].wait_recv()
        if k < swapped:
            x_twin[k].start()
        x_diag[k].start()

    def from_twin(k):
        x_twin[k].wait_recv()
        x_diag[pieces - 1 - k].start()

    with scope('relay'):
        for k in range(DIRECT - swapped):
            relay(k)
    with scope('route_diag'):
        ids_diag.wait_recv()
        route(b_diag)
    with scope('relay'):
        for k in range(DIRECT - swapped, DIRECT):
            from_twin(k - DIRECT + swapped)
            relay(k)
    with scope('norm_across'):
        norm_rows(b_across)
    with scope('wait_diag'):
        all_diag.wait_recv()
    with scope('gather_rest'):
        norm_rows(b_diag)
        gather(b_across)
        gather(b_diag)

    def up_one(e):
        first = pl.multiple_of(e * cap, cap)
        count = blocks * cap
        lhs = jnp.concatenate([rows[b % blocks, pl.ds(first, cap), :] for b in range(2 * blocks)], axis=0)
        slot = e % SLOTS
        gate_act = jnp.dot(lhs, wbuf[slot, 0:kparts].reshape(dim, width), preferred_element_type=jnp.float32)
        up_act = jnp.dot(lhs, wbuf[slot, kparts:2 * kparts].reshape(dim, width), preferred_element_type=jnp.float32)
        hid[e] = (jax.nn.silu(gate_act[0:count]) * up_act[0:count]).astype(jnp.bfloat16)

    def refill(e):
        @pl.when(e < extra)
        def _():
            start_w13(e + SLOTS, 0)

        @pl.when((e > extra) & (e < extra + 2 * num_chunk // per_pair) & ((e - extra) % 2 == 1))
        def _():
            for q in range(per_pair):
                for half in range(2):
                    w2_copy((e - extra) // 2 * per_pair + q, half).start(priority=1)

    def up_step(group):
        def step(i, carry):
            with scope('up_wait'):
                for u in range(group):
                    w_wait((i * group + u) % SLOTS)
            for u in range(group):
                up_one(i * group + u)
            for u in range(group):
                refill(i * group + u)
            return carry
        return step

    fours, pairs = local_exp // 2, local_exp // 4 * 3
    lax.fori_loop(0, fours // 4, up_step(4), 0)
    lax.fori_loop(fours // 2, pairs // 2, up_step(2), 0)
    with scope('gates_rest'):
        gates(b_across)
        gates(b_diag)
    lax.fori_loop(pairs, local_exp, up_step(1), 0)
    for copy in (all_ids, x_mate, all_across, all_twin, all_diag):
        copy.wait_send()

    def d_copy(j):
        return remote(part.at[j, 1 - core], d_recv.at[j], send_sem.at[5], dr_sem.at[j], mate)

    part_rows = num_tok // PARTS

    def x_copy(j, r):
        span = pl.ds(r * part_rows, part_rows)
        return remote(x_send.at[j, span], x_recv.at[j, span], send_sem.at[6], xr_sem.at[j, r], across)

    def y_copy(j, r):
        span = pl.ds(r * part_rows, part_rows)
        return remote(kept.at[j, span], y_recv.at[j, span], send_sem.at[7], yr_sem.at[j], twin)

    def down(j):
        with scope('down_wait'):
            w_wait(w2_slot(j, j % per_pair))
        sub = pl.multiple_of((j % per_pair) * CHUNK, CHUNK)
        for e in range(local_exp):
            w2 = wbuf[w2_slot(j, e // half_exp), e % half_exp, :, pl.ds(sub, CHUNK)]
            lhs = jnp.concatenate([hid[e], hid[e]], axis=0)
            y = jnp.dot(lhs, w2, preferred_element_type=jnp.float32).astype(jnp.bfloat16)
            for b in range(blocks):
                ybuf[b, e * cap:(e + 1) * cap, :] = y[b * cap:(b + 1) * cap, :]

        def mix_block(to_core, to_chip):
            block = CORES * to_chip + to_core
            three = jnp.dot(comb[block], ybuf[block], preferred_element_type=jnp.float32)
            part[j, to_core, to_chip] = (three[0:num_tok] + three[num_tok:2 * num_tok]) + three[2 * num_tok:]

        mix_block(1 - core, 0)
        mix_block(1 - core, 1)
        mix_block(core, 0)
        mix_block(core, 1)
        d_copy(j).start()

    def to_across(i):
        with scope('d_wait'):
            d_copy(i).wait_recv()
        for r in range(PARTS):
            span = pl.ds(r * part_rows, part_rows)
            x_send[i, span] = part[i, core, 1 - chip, span] + d_recv[i, 1 - chip, span]
            x_copy(i, r).start()
        kept[i] = part[i, core, chip] + d_recv[i, chip]

    def to_twin(i):
        for r in range(PARTS):
            with scope('x_wait'):
                x_copy(i, r).wait_recv()
            span = pl.ds(r * part_rows, part_rows)
            kept[i, span] = kept[i, span] + x_recv[i, span]
            y_copy(i, r).start()

    def finish(i):
        with scope('y_wait'):
            remote(kept.at[i], y_recv.at[i], send_sem.at[7], yr_sem.at[i], twin).wait_recv()
        col = pl.multiple_of(i * CHUNK, CHUNK)
        tok = x_all[ep, :, pl.ds(col, CHUNK)].astype(jnp.float32)
        out_ref[:, pl.ds(col, CHUNK)] = (tok + (kept[i] + y_recv[i])).astype(out_ref.dtype)

    def down_step(j, carry):
        @pl.when(j < num_chunk)
        def _():
            down(j)

        @pl.when((j >= LAG_X) & (j < num_chunk + LAG_X))
        def _():
            to_across(j - LAG_X)

        @pl.when((j >= LAG_Y) & (j < num_chunk + LAG_Y))
        def _():
            to_twin(j - LAG_Y)

        @pl.when(j >= LAG_O)
        def _():
            finish(j - LAG_O)

        return carry

    lax.fori_loop(0, num_chunk + LAG_O, down_step, 0)
    remote(d_recv, d_recv, send_sem.at[5], dr_sem.at[0], mate).wait_send()
    remote(x_send, x_recv, send_sem.at[6], xr_sem.at[0, 0], across).wait_send()
    remote(kept, y_recv, send_sem.at[7], yr_sem.at[0], twin).wait_send()


def scoped_kernel(sems, *refs):
    pl.run_scoped(lambda *held: moe_kernel(*refs, *held), *sems)


def moe_call(ep_size, tokens, ids_t, gain, router_t, w_gate, w_up, w_down):
    num_tok, dim = tokens.shape
    top_k = ids_t.shape[0]
    num_exp = router_t.shape[0]
    local_exp, width, _ = w_down.shape
    cap = 2 * top_k * num_tok // num_exp
    kparts = dim // width
    half_exp = local_exp // 2
    chunks = dim // CHUNK
    pieces = num_tok // PIECE
    w_gate = w_gate.reshape(local_exp, kparts, width, width)
    w_up = w_up.reshape(local_exp, kparts, width, width)
    bf16, f32 = jnp.bfloat16, jnp.float32
    vmem = pltpu.VMEM
    dma = pltpu.SemaphoreType.DMA
    any_spec = pl.BlockSpec(memory_space=pl.ANY)
    sems = (
        dma((4,)), dma((SLOTS,)), dma((DIRECT,)), dma((pieces - DIRECT,)), dma((1,)), dma((1,)), dma((3,)),
        dma((chunks,)), dma((chunks, PARTS)), dma((chunks,)), dma((8,)),
    )
    return pl.pallas_call(
        functools.partial(scoped_kernel, sems),
        out_shape=pltpu.VMEM((num_tok, dim), tokens.dtype),
        in_specs=[any_spec] * 7,
        out_specs=pl.BlockSpec(memory_space=pltpu.VMEM),
        scratch_shapes=[
            vmem((ep_size, num_tok, dim), bf16),
            vmem((ep_size, top_k, num_tok), jnp.int32),
            vmem(gain.shape, bf16),
            vmem((num_exp, dim), bf16),
            vmem((SLOTS, half_exp, width, width), bf16),
            vmem((ep_size, num_tok, dim), bf16),
            vmem((ep_size, local_exp * cap, dim), bf16),
            vmem((ep_size, num_exp, num_tok), f32),
            vmem((num_exp, num_tok), f32),
            vmem((ep_size, local_exp * cap, num_tok), bf16),
            vmem((ep_size, 3 * num_tok, local_exp * cap), bf16),
            vmem((local_exp, ep_size * cap, width), bf16),
            vmem((ep_size, local_exp * cap, CHUNK), bf16),
            vmem((chunks, CORES, ep_size // CORES, num_tok, CHUNK), f32),
            vmem((chunks, ep_size // CORES, num_tok, CHUNK), f32),
            vmem((chunks, num_tok, CHUNK), f32),
            vmem((chunks, num_tok, CHUNK), f32),
            vmem((chunks, num_tok, CHUNK), f32),
            vmem((chunks, num_tok, CHUNK), f32),
        ],
        compiler_params=pltpu.CompilerParams(
            collective_id=0, has_side_effects=True, vmem_limit_bytes=VMEM_BYTES),
        name='moe_block',
    )(tokens, ids_t, gain, router_t, w_gate, w_up, w_down)


def solution(mesh):
    ep_size = mesh.shape['ep']
    tok_spec = P(('dp', 'ep'), None)

    def local_block(tokens, expert_ids, norm_gain, router_w, w_gate, w_up, w_down):
        return moe_call(ep_size, tokens, expert_ids.T, norm_gain.reshape(-1, 128), router_w.T, w_gate, w_up, w_down)

    return jax.shard_map(local_block, mesh=mesh, in_specs=(tok_spec, tok_spec, P(None), P(None, None), P('ep', None, 'tp'), P('ep', None, 'tp'), P('ep', 'tp', None)), out_specs=tok_spec, check_vma=False)
```
